512 devices in a mesh: gx: 16 (over y, x), gy: 32 (over z, core).
Axes of the slice: x: 4, y: 4, z: 16, core: 2. Of those that a mesh axis runs over, the one named last changes fastest.
Arguments:
- surface: float32 [1024, 16384], P('gx', 'gy'), may hold values from -6 to 6
- east_velocity: float32 [1024, 16384], P('gx', 'gy'), may hold values from -3 to 3
- north_velocity: float32 [1024, 16384], P('gx', 'gy'), may hold values from -3 to 3
- east_depth: float32 [1024, 16384], P('gx', 'gy'), may hold values from 0.25 to 2
- north_depth: float32 [1024, 16384], P('gx', 'gy'), may hold values from 0.25 to 2
- slot_gauge: int32 [512, 128], P(('gx', 'gy')), may hold values from 0 to 32768, as said below
- slot_cell: int32 [512, 128], P(('gx', 'gy')), may hold values from 0 to 32767
Outputs:
- final_surface: float32 [1024, 16384], P('gx', 'gy')
- final_east: float32 [1024, 16384], P('gx', 'gy')
- final_north: float32 [1024, 16384], P('gx', 'gy')
- gauge_series: float32 [32768, 48], P(('gx', 'gy'))
The draws below stay inside these ranges and needn't reach their ends.
Inputs may be any that keep to these rules, and one draw needn't show every extreme that they name: `slot_gauge`: entries below 32768 are gauge ids: every id 0 to 32767 stands exactly once in the whole array, in the row of the device whose block holds that gauge; the ids owned by device d, d * 64 to (d + 1) * 64 - 1, all lie in blocks with d's gx index. Each row lists its ids first, then 32768 in the unused slots. Some device's row is full in every draw.
All inputs are finite; a program needn't handle non-finite values.
Results may differ from the reference program's by a relative error of at most 0.00012.
Values sent between devices are 32-bit elements; how exact they have to be, the bound alone decides.
No kernel may reach another device: no remote copies, remote signals or barrier semaphores. Data moves between devices by JAX's collectives and lax.ppermute only.
A program may use at most 64 MiB of HBM per device.

```python
import math
import jax
import jax.numpy as jnp

CX = 64
CY = 512
STEPS = 16
SLOTS = 128
GAUGE_DEV = 64
NX = 1024
NY = 16384
GAUGES = 32768
N_GX = 16
N_GY = 32
DEVICES = 512


def draw_slot_gauge(key, part):
    base = jax.random.fold_in(key, 11)
    key_weight, key_busy, key_perm = jax.random.split(base, 3)
    weights = jax.random.randint(key_weight, (N_GX, N_GY), 1, 3)
    busy = jax.random.randint(key_busy, (N_GX,), 0, N_GY)
    column = jnp.arange(N_GY, dtype=jnp.int32)
    is_busy = column[None, :] == busy[:, None]
    weights = jnp.where(is_busy, 0, weights)
    remain = N_GY * GAUGE_DEV - SLOTS
    cumul = jnp.cumsum(weights, axis=1)
    ends = remain * cumul // cumul[:, -1:]
    counts = ends - jnp.concatenate([jnp.zeros((N_GX, 1), jnp.int32), ends[:, :-1]], 1)
    counts = jnp.where(is_busy, SLOTS, counts)
    starts = jnp.cumsum(counts, axis=1) - counts
    band = N_GY * GAUGE_DEV
    perms = jax.vmap(lambda sub: jax.random.permutation(sub, band))(jax.random.split(key_perm, N_GX))
    slot = jnp.arange(SLOTS, dtype=jnp.int32)
    position = jnp.minimum(starts[:, :, None] + slot[None, None, :], band - 1)
    spread = jnp.broadcast_to(perms[:, None, :], (N_GX, N_GY, band))
    picked = jnp.take_along_axis(spread, position, axis=2)
    gauge_ids = jnp.arange(N_GX, dtype=jnp.int32)[:, None, None] * band + picked
    valid = slot[None, None, :] < counts[:, :, None]
    return jnp.where(valid, gauge_ids, GAUGES).reshape(N_GX * N_GY, SLOTS).astype(jnp.int32)


def draw_surface(key, part):
    key_rough = jax.random.fold_in(jax.random.fold_in(key, 23), 0)
    rough = jax.random.normal(key_rough, (NX, NY), jnp.float32)
    return jnp.clip(rough, -6.0, 6.0)


def plant(entries, key, least, top_value):
    shape = entries.shape
    place = [jax.random.randint(jax.random.fold_in(key, axis), (), 0, shape[axis]) for axis in range(len(shape))]
    entries = entries.at[tuple(place)].set(least)
    longest = shape.index(max(shape))
    place[longest] = (place[longest] + 1) % shape[longest]
    return entries.at[tuple(place)].set(top_value)


def shard_levels(key, extent, shards, low, high):
    level, own = 1.0, jax.random.fold_in(key, 6)
    for axis_at, blocks in shards:
        draws = jnp.exp(jax.random.uniform(jax.random.fold_in(own, axis_at), (blocks,), jnp.float32, low / len(shards), high / len(shards)))
        level = level * jnp.repeat(draws, extent[axis_at] // blocks).reshape([-1 if axis == axis_at else 1 for axis in range(len(extent))])
    return level


def bell_draw(rng, extent, deviation, most, cuts=(), kind=jnp.bfloat16):
    values = deviation * jax.random.normal(rng, extent, jnp.float32)
    if cuts:
        values = values * shard_levels(rng, extent, cuts, -0.22, 0.18)
    return jnp.clip(values, -most, most).astype(kind)


def setup_inputs(seed: int = 0) -> dict:
    keys = jax.random.split(jax.random.key(seed), 8)
    return {
        "surface": draw_surface(jax.random.fold_in(keys[7], 71), 0),
        "east_velocity": bell_draw(keys[1], (NX, NY), 0.5, 3.0, ((0, 16), (1, 32)), jnp.float32),
        "north_velocity": bell_draw(keys[2], (NX, NY), 0.5, 3.0, ((0, 16), (1, 32)), jnp.float32),
        "east_depth": jnp.clip(jnp.exp(math.log(2.0) - 2.0794415 * jax.random.uniform(keys[3], (NX, NY), jnp.float32) ** shard_levels(keys[3], (NX, NY), ((0, 16), (1, 32)), -0.2, 0.2)), 0.25, 2.0),
        "north_depth": jnp.clip(jnp.exp(math.log(2.0) - 2.0794415 * jax.random.uniform(keys[4], (NX, NY), jnp.float32) ** shard_levels(keys[4], (NX, NY), ((0, 16), (1, 32)), -0.2, 0.2)), 0.25, 2.0),
        "slot_gauge": draw_slot_gauge(jax.random.fold_in(keys[7], 71), 0),
        "slot_cell": plant(jax.random.randint(keys[6], (DEVICES, SLOTS), 0, CX * CY), jax.random.fold_in(keys[6], 1), 0, (CX * CY) - 1).astype(jnp.int32),
    }


time_step = 0.45


def advance(eta, east, north, east_depth, north_depth):
    eta_down = jnp.concatenate([eta[1:], jnp.zeros_like(eta[:1])], 0)
    eta_right = jnp.concatenate([eta[:, 1:], jnp.zeros_like(eta[:, :1])], 1)
    east = east - time_step * (eta_down - eta)
    north = north - time_step * (eta_right - eta)
    flux_x = east_depth * east
    flux_y = north_depth * north
    flux_up = jnp.concatenate([jnp.zeros_like(flux_x[:1]), flux_x[:-1]], 0)
    flux_left = jnp.concatenate([jnp.zeros_like(flux_y[:, :1]), flux_y[:, :-1]], 1)
    eta = eta - time_step * (flux_x - flux_up + flux_y - flux_left)
    return eta, east, north


def reference(surface, east_velocity, north_velocity, east_depth, north_depth, slot_gauge, slot_cell):
    device = jnp.arange(slot_gauge.shape[0], dtype=jnp.int32)[:, None]
    grid_rows = ((device // N_GY) * CX + slot_cell // CY).reshape(-1).astype(jnp.int32)
    grid_cols = ((device % N_GY) * CY + slot_cell % CY).reshape(-1).astype(jnp.int32)
    eta, east, north = surface, east_velocity, north_velocity
    records = []
    for step in range(STEPS):
        eta, east, north = advance(eta, east, north, east_depth, north_depth)
        records.append(jnp.stack([eta[grid_rows, grid_cols], east[grid_rows, grid_cols], north[grid_rows, grid_cols]]))
    stacked = jnp.stack(records)
    flat = jnp.transpose(stacked, (2, 1, 0)).reshape(grid_rows.shape[0], 3 * STEPS)
    holder = jnp.zeros((GAUGES + 1, 3 * STEPS), flat.dtype)
    series = holder.at[slot_gauge.reshape(-1).astype(jnp.int32)].set(flat)[:GAUGES]
    return eta, east, north, series
```

```python
import functools

import jax
import jax.numpy as jnp
from jax import lax
from jax.experimental import pallas as pl
from jax.experimental.pallas import tpu as pltpu
from jax.sharding import PartitionSpec as P

STEPS = 16
GAUGE_DEV = 64
QUAD = 4
LANES = 128
DT = 0.45


def lane_ids(shape):
    return lax.broadcasted_iota(jnp.int32, shape, 1)


def pack_columns_kernel(e, u, v, dx, dy, top, bot, head, tail, *, margin):
    rows, cols = e.shape
    lane = lane_ids((margin, LANES))
    last = cols - LANES
    fields = (e, u, v, dx, dy)
    for r in range(0, rows + 2 * margin, margin):
        out_head = jnp.zeros((margin, LANES), jnp.float32)
        out_tail = jnp.zeros((margin, LANES), jnp.float32)
        for f, ref in enumerate(fields):
            if r == 0:
                src, at = top, f * margin
            elif r == rows + margin:
                src, at = bot, f * margin
            else:
                src, at = ref, r - margin
            first = src[at : at + margin, :LANES]
            final = src[at : at + margin, last:]
            mine = (lane >= margin * f) & (lane < margin * (f + 1))
            if f:
                first = pltpu.roll(first, margin * f, 1)
            final = pltpu.roll(final, (margin * f + margin) % LANES, 1)
            out_head = jnp.where(mine, first, out_head)
            out_tail = jnp.where(mine, final, out_tail)
        head[r : r + margin, :] = out_head
        tail[r : r + margin, :] = out_tail


def steps_kernel(
    cells, edges, ids, e, u, v, dx, dy, top, bot, from_left, from_right,
    out_e, out_u, out_v, out_rec, he, hu, hv, sx, sy, *, steps,
):
    rows, cols = e.shape
    margin = steps
    own = cols // LANES
    tiles = own + 1
    height = rows + 2 * margin
    pitch = height + 8
    chunk = 16
    lane = lane_ids((chunk, LANES))

    for f, (ref, dst, base) in enumerate(
        ((e, he, 0), (u, hu, 0), (v, hv, 0), (dx, sx, 8), (dy, sy, 8))
    ):
        for j in range(own):
            cut = slice(LANES * j, LANES * (j + 1))
            dst[j, base : base + margin, :] = top[f * margin : (f + 1) * margin, cut]
            dst[j, base + margin : base + margin + rows, :] = ref[:, cut]
            dst[j, base + margin + rows : base + height, :] = bot[f * margin : (f + 1) * margin, cut]
        for r in range(0, height, chunk):
            right = from_right[r : r + chunk, :]
            left = from_left[r : r + chunk, :]
            if f:
                right = pltpu.roll(right, LANES - margin * f, 1)
            left = pltpu.roll(left, (LANES - margin - margin * f) % LANES, 1)
            tile = jnp.where(
                lane < margin, right, jnp.where(lane >= LANES - margin, left, jnp.zeros_like(left))
            )
            dst[own, base + r : base + r + chunk, :] = tile

    keep_rows = edges[0] == 0
    keep_cols = (lane >= LANES // 2) | (edges[1] == 0)

    for s in range(steps):
        low = (s // 8) * 8
        high = height - low
        now, new = s * pitch, (s + 1) * pitch
        for r in range(low, high, chunk):
            size = min(chunk, high - r)
            at_edge = lane[:size] == LANES - 1
            eta = [he[j, now + r : now + r + size, :] for j in range(tiles)]
            turned = [pltpu.roll(t, LANES - 1, 1) for t in eta]
            for j in range(tiles):
                down = he[j, now + r + 1 : now + r + 1 + size, :]
                right = jnp.where(at_edge, turned[(j + 1) % tiles], turned[j])
                hu[j, new + r : new + r + size, :] = hu[j, now + r : now + r + size, :] - DT * (
                    down - eta[j]
                )
                hv[j, new + r : new + r + size, :] = hv[j, now + r : now + r + size, :] - DT * (
                    right - eta[j]
                )
        for r in range(low, high, chunk):
            size = min(chunk, high - r)
            at_edge = lane[:size] == 0
            flux_y = [
                sy[j, 8 + r : 8 + r + size, :] * hv[j, new + r : new + r + size, :]
                for j in range(tiles)
            ]
            turned = [pltpu.roll(t, 1, 1) for t in flux_y]
            for j in range(tiles):
                flux_x = sx[j, 8 + r : 8 + r + size, :] * hu[j, new + r : new + r + size, :]
                flux_up = (
                    sx[j, 7 + r : 7 + r + size, :] * hu[j, new + r - 1 : new + r - 1 + size, :]
                )
                flux_left = jnp.where(at_edge, turned[(j - 1) % tiles], turned[j])
                eta = he[j, now + r : now + r + size, :] - DT * (
                    flux_x - flux_up + flux_y[j] - flux_left
                )
                if j == own:
                    eta = jnp.where(keep_cols[:size], eta, 0.0)
                if r >= rows + margin:
                    eta = jnp.where(keep_rows, eta, 0.0)
                elif r + size > rows + margin:
                    split = rows + margin - r
                    row = lax.broadcasted_iota(jnp.int32, (size, LANES), 0)
                    eta = jnp.where((row < split) | keep_rows, eta, 0.0)
                he[j, new + r : new + r + size, :] = eta

    last = steps * pitch + margin
    for out, hist in ((out_e, he), (out_u, hu), (out_v, hv)):
        for j in range(own):
            out[:, LANES * j : LANES * (j + 1)] = hist[j, last : last + rows, :]

    lane8 = lane_ids((8, LANES))
    count = cells.shape[1]

    def one_slot(k, kept):
        cell = cells[0, k]
        row = cell // cols
        col = cell % cols
        j = col // LANES
        shift = (k - col % LANES) % LANES
        out = []
        mine = lane8 == k
        for q, hist in enumerate((he, hu, hv)):
            for h in range(steps // 8):
                tile = hist[j, pl.ds((8 * h + 1) * pitch + margin + row, 8, stride=pitch), :]
                turned = pltpu.roll(tile, shift, 1)
                out.append(jnp.where(mine, turned, kept[q * (steps // 8) + h]))
        return tuple(out)

    zero = jnp.zeros((8, LANES), jnp.float32)
    kept = lax.fori_loop(0, count, one_slot, (zero,) * (3 * steps // 8), unroll=8)
    for t, tile in enumerate(kept):
        out_rec[8 * t : 8 * t + 8, :] = tile
    out_rec[3 * steps : 3 * steps + 8, :] = jnp.broadcast_to(ids[...].astype(jnp.float32), (8, LANES))


def place_kernel(base, rec, out, *, series, members):
    sources, _, slots = rec.shape
    gauges = members * GAUGE_DEV
    records = jnp.concatenate([rec[k, :series, :] for k in range(sources)], axis=1)
    one = records.astype(jnp.bfloat16)
    rest = records - one.astype(jnp.float32)
    two = rest.astype(jnp.bfloat16)
    three = (rest - two.astype(jnp.float32)).astype(jnp.bfloat16)
    terms = jnp.concatenate([one, two, three], axis=0)
    number = lax.broadcasted_iota(jnp.int32, (gauges, slots), 0)
    wanted = base[0] + (number // GAUGE_DEV) * (sources * GAUGE_DEV) + number % GAUGE_DEV
    wanted = wanted.astype(jnp.float32)
    picks = [
        (rec[k, series : series + 1, :] == wanted).astype(jnp.float32).astype(jnp.bfloat16)
        for k in range(sources)
    ]
    pick = jnp.concatenate(picks, axis=1)
    full = lax.dot_general(terms, pick, (((1,), (1,)), ((), ())), preferred_element_type=jnp.float32)
    dense = full[:series] + full[series : 2 * series] + full[2 * series :]
    half = series // 2
    low = lane_ids((half, LANES)) < GAUGE_DEV
    for t in range(gauges // LANES):
        tile = dense[:, LANES * t : LANES * (t + 1)]
        turned = pltpu.roll(tile, GAUGE_DEV, 1)
        out[2 * t] = jnp.where(low, tile[:half], turned[half:])
        out[2 * t + 1] = jnp.where(low, turned[:half], tile[half:])


def finish_kernel(parts, out, *, series):
    total = parts[0]
    for k in range(1, parts.shape[0]):
        total = total + parts[k]
    turned = pltpu.roll(total, GAUGE_DEV, 1)
    pad = jnp.zeros((LANES - series, LANES), jnp.float32)
    square = jnp.concatenate([total, turned, pad], axis=0)
    out[...] = jnp.transpose(square)[:GAUGE_DEV, :series]


def in_vmem(count):
    return [pl.BlockSpec(memory_space=pltpu.VMEM)] * count


def in_smem(count):
    return [pl.BlockSpec(memory_space=pltpu.SMEM)] * count


def f32(*shape):
    return jax.ShapeDtypeStruct(shape, jnp.float32)


def shards(surface, east, north, east_depth, north_depth, slot_gauge, slot_cell):
    rows, cols = surface.shape
    margin = STEPS
    series = 3 * STEPS
    n_gx, n_gy = lax.axis_size("gx"), lax.axis_size("gy")
    a, b = lax.axis_index("gx"), lax.axis_index("gy")
    fields = (surface, east, north, east_depth, north_depth)

    def shifted(tail, head, axis, count):
        from_before = lax.ppermute(tail, axis, [(i, i + 1) for i in range(count - 1)])
        from_after = lax.ppermute(head, axis, [(i + 1, i) for i in range(count - 1)])
        return from_before, from_after

    head_rows = jnp.concatenate([f[:margin] for f in fields], axis=0)
    tail_rows = jnp.concatenate([f[rows - margin :] for f in fields], axis=0)
    top, bot = shifted(tail_rows, head_rows, "gx", n_gx)

    height = rows + 2 * margin
    head, tail = pl.pallas_call(
        functools.partial(pack_columns_kernel, margin=margin),
        out_shape=(f32(height, LANES), f32(height, LANES)),
        in_specs=in_vmem(7),
        out_specs=tuple(in_vmem(2)),
        name="pack_columns",
    )(*fields, top, bot)
    from_left, from_right = shifted(tail, head, "gy", n_gy)

    tiles = cols // LANES + 1
    pitch = height + 8
    history = pltpu.VMEM((tiles, (STEPS + 1) * pitch, LANES), jnp.float32)
    depth = pltpu.VMEM((tiles, pitch, LANES), jnp.float32)
    edges = jnp.stack([a == n_gx - 1, b == n_gy - 1]).astype(jnp.int32)
    eta, u, v, rec = pl.pallas_call(
        functools.partial(steps_kernel, steps=STEPS),
        out_shape=(f32(rows, cols), f32(rows, cols), f32(rows, cols), f32(series + 8, LANES)),
        in_specs=in_smem(2) + in_vmem(10),
        out_specs=tuple(in_vmem(4)),
        scratch_shapes=[history, history, history, depth, depth],
        name="leapfrog",
    )(slot_cell, edges, slot_gauge, *fields, top, bot, from_left, from_right)

    near = [[QUAD * i + j for j in range(QUAD)] for i in range(n_gy // QUAD)]
    members = n_gy // QUAD
    far = [[i + QUAD * j for j in range(members)] for i in range(QUAD)]
    gathered = lax.all_gather(rec, "gy", axis_index_groups=near)
    base = (a * (n_gy * GAUGE_DEV) + (b % QUAD) * GAUGE_DEV).astype(jnp.int32).reshape(1)
    half = series // 2
    placed = pl.pallas_call(
        functools.partial(place_kernel, series=series, members=members),
        out_shape=f32(members, half, LANES),
        in_specs=in_smem(1) + in_vmem(1),
        out_specs=in_vmem(1)[0],
        name="place",
    )(base, gathered)
    arrived = lax.all_to_all(placed, "gy", 0, 0, axis_index_groups=far, tiled=True)
    out = pl.pallas_call(
        functools.partial(finish_kernel, series=series),
        out_shape=f32(GAUGE_DEV, series),
        in_specs=in_vmem(1),
        out_specs=in_vmem(1)[0],
        name="finish",
    )(arrived)
    return eta, u, v, out


def solution(mesh):
    block = P("gx", "gy")
    rows = P(("gx", "gy"), None)
    return jax.shard_map(
        shards,
        mesh=mesh,
        in_specs=(block,) * 5 + (rows, rows),
        out_specs=(block,) * 3 + (rows,),
        check_vma=False,
    )
```

```python
import functools

import jax
import jax.numpy as jnp
from jax import lax
from jax.experimental import pallas as pl
from jax.experimental.pallas import tpu as pltpu
from jax.sharding import PartitionSpec as P

STEPS = 16
GAUGE_DEV = 64
QUAD = 4
LANES = 128
DT = 0.45
MIB = 1 << 20


def lane_ids(shape):
    return lax.broadcasted_iota(jnp.int32, shape, 1)


def pack_columns_kernel(e, u, v, dx, dy, top, bot, head, tail, *, margin):
    rows, cols = e.shape
    lane = lane_ids((margin, LANES))
    last = cols - LANES
    fields = (e, u, v, dx, dy)
    for r in range(0, rows + 2 * margin, margin):
        out_head = jnp.zeros((margin, LANES), jnp.float32)
        out_tail = jnp.zeros((margin, LANES), jnp.float32)
        for f, ref in enumerate(fields):
            if r == 0:
                src, at = top, f * margin
            elif r == rows + margin:
                src, at = bot, f * margin
            else:
                src, at = ref, r - margin
            first = src[at : at + margin, :LANES]
            final = src[at : at + margin, last:]
            mine = (lane >= margin * f) & (lane < margin * (f + 1))
            if f:
                first = pltpu.roll(first, margin * f, 1)
            final = pltpu.roll(final, (margin * f + margin) % LANES, 1)
            out_head = jnp.where(mine, first, out_head)
            out_tail = jnp.where(mine, final, out_tail)
        head[r : r + margin, :] = out_head
        tail[r : r + margin, :] = out_tail


def pack_rows_kernel(e, u, v, dx, dy, head, tail, sems, *, margin):
    rows = e.shape[0]
    copies = []
    for f, ref in enumerate((e, u, v, dx, dy)):
        place = pl.ds(margin * f, margin)
        copies.append(pltpu.make_async_copy(ref.at[pl.ds(0, margin), :], head.at[place, :], sems.at[f]))
        copies.append(
            pltpu.make_async_copy(ref.at[pl.ds(rows - margin, margin), :], tail.at[place, :], sems.at[5 + f])
        )
    for copy in copies:
        copy.start()
    for copy in copies:
        copy.wait()


def steps_kernel(
    cells_in, place_x, place_y, ids_in, e, u, v, dx, dy, top, bot, from_left, from_right,
    out_e, out_u, out_v, out_rec, he, hu, hv, sx, sy, cells, ids, staged, list_sems, out_sems,
    *, steps, last_x, last_y,
):
    rows, cols = e.shape
    margin = steps
    own = cols // LANES
    tiles = own + 1
    height = rows + 2 * margin
    pitch = height + 8
    chunk = 16
    lane = lane_ids((chunk, LANES))
    lists = [
        pltpu.make_async_copy(cells_in, cells, list_sems.at[0]),
        pltpu.make_async_copy(ids_in, ids, list_sems.at[1]),
    ]
    for copy in lists:
        copy.start()

    for f, (ref, dst, factor) in enumerate(
        ((e, he, DT), (u, hu, None), (v, hv, None), (dx, sx, DT * DT), (dy, sy, DT * DT))
    ):
        def scaled(value):
            return value if factor is None else value * factor

        for j in range(own):
            cut = slice(LANES * j, LANES * (j + 1))
            dst[j, :margin, :] = scaled(top[f * margin : (f + 1) * margin, cut])
            dst[j, margin : margin + rows, :] = scaled(ref[:, cut])
            dst[j, margin + rows : height, :] = scaled(bot[f * margin : (f + 1) * margin, cut])
        for r in range(0, height, chunk):
            right = from_right[r : r + chunk, :]
            left = from_left[r : r + chunk, :]
            if f:
                right = pltpu.roll(right, LANES - margin * f, 1)
            left = pltpu.roll(left, (LANES - margin - margin * f) % LANES, 1)
            tile = jnp.where(
                lane < margin, right, jnp.where(lane >= LANES - margin, left, jnp.zeros_like(left))
            )
            dst[own, r : r + chunk, :] = scaled(tile)

    size = 8
    lane8 = lane_ids((size, LANES))
    row8 = lax.broadcasted_iota(jnp.int32, (size, LANES), 0)
    first_lane, final_lane, final_row = lane8 == 0, lane8 == LANES - 1, row8 == size - 1
    keep_rows = place_x[0] != last_x
    keep_cols = (lane8 >= LANES // 2) | (place_y[0] != last_y)

    for s in range(steps):
        low = (s // size) * size
        now, new = s * pitch, (s + 1) * pitch
        flux_before = [None] * tiles
        for r in range(low, height - low, size):
            eta = [he[j, now + r : now + r + size, :] for j in range(tiles)]
            flux_y = []
            for j in range(tiles):
                right = pltpu.roll(jnp.where(first_lane, eta[(j + 1) % tiles], eta[j]), LANES - 1, 1)
                north = hv[j, now + r : now + r + size, :] - (right - eta[j])
                hv[j, new + r : new + r + size, :] = north
                flux_y.append(sy[j, r : r + size, :] * north)
            for j in range(tiles):
                down = he[j, now + r + 1 : now + r + 1 + size, :]
                east = hu[j, now + r : now + r + size, :] - (down - eta[j])
                hu[j, new + r : new + r + size, :] = east
                flux_x = sx[j, r : r + size, :] * east
                above = flux_x if flux_before[j] is None else flux_before[j]
                flux_up = pltpu.roll(jnp.where(final_row, above, flux_x), 1, 0)
                flux_before[j] = flux_x
                flux_left = pltpu.roll(jnp.where(final_lane, flux_y[(j - 1) % tiles], flux_y[j]), 1, 1)
                after = eta[j] - ((flux_x - flux_up) + (flux_y[j] - flux_left))
                if j == own:
                    after = jnp.where(keep_cols, after, 0.0)
                if r >= rows + margin:
                    after = jnp.where(keep_rows, after, 0.0)
                he[j, new + r : new + r + size, :] = after

    last = steps * pitch + margin
    outs = []
    for j in range(own):
        cut = pl.ds(LANES * j, LANES)
        outs.append(pltpu.make_async_copy(hu.at[j, pl.ds(last, rows), :], out_u.at[:, cut], out_sems.at[j]))
        outs.append(
            pltpu.make_async_copy(hv.at[j, pl.ds(last, rows), :], out_v.at[:, cut], out_sems.at[own + j])
        )
    outs.append(pltpu.make_async_copy(staged, out_e, out_sems.at[2 * own]))
    for copy in outs[:-1]:
        copy.start()
    for j in range(own):
        staged[:, LANES * j : LANES * (j + 1)] = he[j, last : last + rows, :] * (1.0 / DT)
    outs[-1].start()
    for copy in lists:
        copy.wait()

    count = cells.shape[1]
    groups = steps // size

    def one_slot(k, kept):
        cell = cells[0, k]
        row = cell >> (cols.bit_length() - 1)
        col = cell & (cols - 1)
        j = col >> (LANES.bit_length() - 1)
        shift = (k - col) & (LANES - 1)
        out = []
        mine = lane8 == k
        for q, hist in enumerate((he, hu, hv)):
            for h in range(groups):
                tile = hist[j, pl.ds((size * h + 1) * pitch + margin + row, size, stride=pitch), :]
                turned = pltpu.roll(tile, shift, 1)
                out.append(jnp.where(mine, turned, kept[q * groups + h]))
        return tuple(out)

    zero = jnp.zeros((size, LANES), jnp.float32)
    kept = lax.fori_loop(0, count, one_slot, (zero,) * (3 * groups), unroll=32)
    for t, tile in enumerate(kept):
        out_rec[size * t : size * (t + 1), :] = tile * (1.0 / DT) if t < groups else tile
    out_rec[3 * steps : 3 * steps + 8, :] = jnp.broadcast_to(ids[...].astype(jnp.float32), (8, LANES))
    for copy in outs:
        copy.wait()


def place_kernel(base, rec, out, *, series, members):
    sources, _, slots = rec.shape
    gauges = members * GAUGE_DEV
    records = jnp.concatenate([rec[k, :series, :] for k in range(sources)], axis=1)
    one = records.astype(jnp.bfloat16)
    rest = records - one.astype(jnp.float32)
    two = rest.astype(jnp.bfloat16)
    three = (rest - two.astype(jnp.float32)).astype(jnp.bfloat16)
    terms = jnp.concatenate([one, two, three], axis=0)
    number = lax.broadcasted_iota(jnp.int32, (gauges, slots), 0)
    wanted = base[0] + (number // GAUGE_DEV) * (sources * GAUGE_DEV) + number % GAUGE_DEV
    wanted = wanted.astype(jnp.float32)
    picks = [
        (rec[k, series : series + 1, :] == wanted).astype(jnp.float32).astype(jnp.bfloat16)
        for k in range(sources)
    ]
    pick = jnp.concatenate(picks, axis=1)
    full = lax.dot_general(terms, pick, (((1,), (1,)), ((), ())), preferred_element_type=jnp.float32)
    dense = full[:series] + full[series : 2 * series] + full[2 * series :]
    half = series // 2
    low = lane_ids((half, LANES)) < GAUGE_DEV
    for t in range(gauges // LANES):
        tile = dense[:, LANES * t : LANES * (t + 1)]
        turned = pltpu.roll(tile, GAUGE_DEV, 1)
        out[2 * t] = jnp.where(low, tile[:half], turned[half:])
        out[2 * t + 1] = jnp.where(low, turned[:half], tile[half:])


def finish_kernel(parts, out, *, series):
    total = parts[0]
    for k in range(1, parts.shape[0]):
        total = total + parts[k]
    turned = pltpu.roll(total, GAUGE_DEV, 1)
    out[: series // 2, :] = total[:, :GAUGE_DEV]
    out[series // 2 :, :] = turned[:, :GAUGE_DEV]


def in_vmem(count):
    return [pl.BlockSpec(memory_space=pltpu.VMEM)] * count


def in_smem(count):
    return [pl.BlockSpec(memory_space=pltpu.SMEM)] * count


def f32(*shape):
    return jax.ShapeDtypeStruct(shape, jnp.float32)


def shards(surface, east, north, east_depth, north_depth, slot_gauge, slot_cell):
    rows, cols = surface.shape
    margin = STEPS
    series = 3 * STEPS
    n_gx, n_gy = lax.axis_size("gx"), lax.axis_size("gy")
    a, b = lax.axis_index("gx"), lax.axis_index("gy")
    fields = (surface, east, north, east_depth, north_depth)

    def shifted(tail, head, axis, count):
        from_before = lax.ppermute(tail, axis, [(i, i + 1) for i in range(count - 1)])
        from_after = lax.ppermute(head, axis, [(i + 1, i) for i in range(count - 1)])
        return from_before, from_after

    whole = pl.BlockSpec(memory_space=pltpu.HBM)
    head_rows, tail_rows = pl.pallas_call(
        functools.partial(pack_rows_kernel, margin=margin),
        out_shape=(f32(5 * margin, cols), f32(5 * margin, cols)),
        in_specs=[whole] * 5,
        out_specs=tuple(in_vmem(2)),
        scratch_shapes=[pltpu.SemaphoreType.DMA((10,))],
        compiler_params=pltpu.CompilerParams(vmem_limit_bytes=4 * MIB),
        name="pack_rows",
    )(*(pltpu.with_memory_space_constraint(f, pltpu.HBM) for f in fields))
    top, bot = shifted(tail_rows, head_rows, "gx", n_gx)

    height = rows + 2 * margin
    head, tail = pl.pallas_call(
        functools.partial(pack_columns_kernel, margin=margin),
        out_shape=(f32(height, LANES), f32(height, LANES)),
        in_specs=in_vmem(7),
        out_specs=tuple(in_vmem(2)),
        compiler_params=pltpu.CompilerParams(vmem_limit_bytes=4 * MIB),
        name="pack_columns",
    )(*fields, top, bot)
    from_left, from_right = shifted(tail, head, "gy", n_gy)

    tiles = cols // LANES + 1
    pitch = height + 8
    history = pltpu.VMEM((tiles, (STEPS + 1) * pitch, LANES), jnp.float32)
    depth = pltpu.VMEM((tiles, height, LANES), jnp.float32)
    eta, u, v, rec = pl.pallas_call(
        functools.partial(steps_kernel, steps=STEPS, last_x=n_gx - 1, last_y=n_gy - 1),
        out_shape=(f32(rows, cols), f32(rows, cols), f32(rows, cols), f32(series + 8, LANES)),
        in_specs=[whole] + in_smem(2) + [whole] + in_vmem(9),
        out_specs=(whole,) * 3 + tuple(in_vmem(1)),
        scratch_shapes=[
            history, history, history, depth, depth,
            pltpu.SMEM(slot_cell.shape, jnp.int32),
            pltpu.VMEM(slot_gauge.shape, jnp.int32),
            pltpu.VMEM((rows, cols), jnp.float32),
            pltpu.SemaphoreType.DMA((2,)),
            pltpu.SemaphoreType.DMA((2 * tiles - 1,)),
        ],
        compiler_params=pltpu.CompilerParams(vmem_limit_bytes=24 * MIB),
        name="leapfrog",
    )(
        pltpu.with_memory_space_constraint(slot_cell, pltpu.HBM),
        a.astype(jnp.int32).reshape(1),
        b.astype(jnp.int32).reshape(1),
        pltpu.with_memory_space_constraint(slot_gauge, pltpu.HBM),
        *fields, top, bot, from_left, from_right,
    )

    near = [[QUAD * i + j for j in range(QUAD)] for i in range(n_gy // QUAD)]
    members = n_gy // QUAD
    far = [[i + QUAD * j for j in range(members)] for i in range(QUAD)]
    gathered = lax.all_gather(rec, "gy", axis_index_groups=near)
    base = (a * (n_gy * GAUGE_DEV) + (b % QUAD) * GAUGE_DEV).astype(jnp.int32).reshape(1)
    half = series // 2
    placed = pl.pallas_call(
        functools.partial(place_kernel, series=series, members=members),
        out_shape=f32(members, half, LANES),
        in_specs=in_smem(1) + in_vmem(1),
        out_specs=in_vmem(1)[0],
        compiler_params=pltpu.CompilerParams(vmem_limit_bytes=8 * MIB),
        name="place",
    )(base, gathered)
    arrived = lax.all_to_all(placed, "gy", 0, 0, axis_index_groups=far, tiled=True)
    out = pl.pallas_call(
        functools.partial(finish_kernel, series=series),
        out_shape=f32(series, GAUGE_DEV),
        in_specs=in_vmem(1),
        out_specs=in_vmem(1)[0],
        compiler_params=pltpu.CompilerParams(vmem_limit_bytes=4 * MIB),
        name="finish",
    )(arrived)
    return eta, u, v, out.T


def solution(mesh):
    block = P("gx", "gy")
    rows = P(("gx", "gy"), None)
    return jax.shard_map(
        shards,
        mesh=mesh,
        in_specs=(block,) * 5 + (rows, rows),
        out_specs=(block,) * 3 + (rows,),
        check_vma=False,
    )
```

```python
import functools

import jax
import jax.numpy as jnp
from jax import lax
from jax.experimental import pallas as pl
from jax.experimental.pallas import tpu as pltpu
from jax.sharding import PartitionSpec as P

STEPS = 16
GAUGE_DEV = 64
QUAD = 2
LANES = 128
DT = 0.45
MIB = 1 << 20


def lane_ids(shape):
    return lax.broadcasted_iota(jnp.int32, shape, 1)


def pack_columns_kernel(e, u, v, dx, dy, top, bot, head, tail, *, margin):
    rows, cols = e.shape
    lane = lane_ids((margin, LANES))
    last = cols - LANES
    fields = (e, u, v, dx, dy)
    for r in range(0, rows + 2 * margin, margin):
        out_head = jnp.zeros((margin, LANES), jnp.float32)
        out_tail = jnp.zeros((margin, LANES), jnp.float32)
        for f, ref in enumerate(fields):
            if r == 0:
                src, at = top, f * margin
            elif r == rows + margin:
                src, at = bot, f * margin
            else:
                src, at = ref, r - margin
            first = src[at : at + margin, :LANES]
            final = src[at : at + margin, last:]
            mine = (lane >= margin * f) & (lane < margin * (f + 1))
            if f:
                first = pltpu.roll(first, margin * f, 1)
            final = pltpu.roll(final, (margin * f + margin) % LANES, 1)
            out_head = jnp.where(mine, first, out_head)
            out_tail = jnp.where(mine, final, out_tail)
        head[r : r + margin, :] = out_head
        tail[r : r + margin, :] = out_tail


def pack_rows_kernel(e, u, v, dx, dy, head, tail, sems, *, margin):
    rows = e.shape[0]
    copies = []
    for f, ref in enumerate((e, u, v, dx, dy)):
        place = pl.ds(margin * f, margin)
        copies.append(pltpu.make_async_copy(ref.at[pl.ds(0, margin), :], head.at[place, :], sems.at[f]))
        copies.append(
            pltpu.make_async_copy(ref.at[pl.ds(rows - margin, margin), :], tail.at[place, :], sems.at[5 + f])
        )
    for copy in copies:
        copy.start()
    for copy in copies:
        copy.wait()


def steps_kernel(
    cells_in, place_x, place_y, ids_in, e, u, v, dx, dy, top, bot, from_left, from_right,
    out_e, out_u, out_v, out_rec, he, hu, hv, sx, sy, cells, ids, list_sems,
    *, steps, last_x, last_y,
):
    rows, cols = e.shape
    margin = steps
    own = cols // LANES
    tiles = own + 1
    height = rows + 2 * margin
    pitch = height + 8
    chunk = 16
    lane = lane_ids((chunk, LANES))
    lists = [
        pltpu.make_async_copy(cells_in, cells, list_sems.at[0]),
        pltpu.make_async_copy(ids_in, ids, list_sems.at[1]),
    ]
    for copy in lists:
        copy.start()

    for f, (ref, dst, factor) in enumerate(
        ((e, he, DT), (u, hu, None), (v, hv, None), (dx, sx, DT * DT), (dy, sy, DT * DT))
    ):
        def scaled(value):
            return value if factor is None else value * factor

        for j in range(own):
            cut = slice(LANES * j, LANES * (j + 1))
            dst[j, :margin, :] = scaled(top[f * margin : (f + 1) * margin, cut])
            dst[j, margin : margin + rows, :] = scaled(ref[:, cut])
            dst[j, margin + rows : height, :] = scaled(bot[f * margin : (f + 1) * margin, cut])
        for r in range(0, height, chunk):
            right = from_right[r : r + chunk, :]
            left = from_left[r : r + chunk, :]
            if f:
                right = pltpu.roll(right, LANES - margin * f, 1)
            left = pltpu.roll(left, (LANES - margin - margin * f) % LANES, 1)
            tile = jnp.where(
                lane < margin, right, jnp.where(lane >= LANES - margin, left, jnp.zeros_like(left))
            )
            dst[own, r : r + chunk, :] = scaled(tile)

    size = 8
    lane8 = lane_ids((size, LANES))
    row8 = lax.broadcasted_iota(jnp.int32, (size, LANES), 0)
    first_lane, final_lane, final_row = lane8 == 0, lane8 == LANES - 1, row8 == size - 1
    keep_rows = place_x[0] != last_x
    keep_cols = (lane8 >= LANES // 2) | (place_y[0] != last_y)

    def one_step(low, s):
        now = pl.multiple_of(s * pitch, 8)
        new = pl.multiple_of(now + pitch, 8)
        flux_before = [None] * tiles
        for r in range(low, height - low, size):
            eta = [he[j, pl.ds(now + r, size), :] for j in range(tiles)]
            flux_y = []
            for j in range(tiles):
                right = pltpu.roll(jnp.where(first_lane, eta[(j + 1) % tiles], eta[j]), LANES - 1, 1)
                north = hv[j, pl.ds(now + r, size), :] - (right - eta[j])
                hv[j, pl.ds(new + r, size), :] = north
                flux_y.append(sy[j, r : r + size, :] * north)
            for j in range(tiles):
                down = he[j, pl.ds(now + r + 1, size), :]
                east = hu[j, pl.ds(now + r, size), :] - (down - eta[j])
                hu[j, pl.ds(new + r, size), :] = east
                flux_x = sx[j, r : r + size, :] * east
                above = flux_x if flux_before[j] is None else flux_before[j]
                flux_up = pltpu.roll(jnp.where(final_row, above, flux_x), 1, 0)
                flux_before[j] = flux_x
                flux_left = pltpu.roll(jnp.where(final_lane, flux_y[(j - 1) % tiles], flux_y[j]), 1, 1)
                after = eta[j] - ((flux_x - flux_up) + (flux_y[j] - flux_left))
                if j == own:
                    after = jnp.where(keep_cols, after, 0.0)
                if r >= rows + margin:
                    after = jnp.where(keep_rows, after, 0.0)
                he[j, pl.ds(new + r, size), :] = after

    for low in range(0, steps, size):
        lax.fori_loop(low, low + size, lambda s, _: one_step(low, s), None, unroll=1)

    last = steps * pitch + margin
    for out, hist, factor in ((out_e, he, 1.0 / DT), (out_u, hu, None), (out_v, hv, None)):
        for j in range(own):
            value = hist[j, last : last + rows, :]
            out[:, LANES * j : LANES * (j + 1)] = value if factor is None else value * factor
    for copy in lists:
        copy.wait()

    count = cells.shape[1]
    groups = steps // size

    def one_slot(k, kept):
        cell = cells[0, k]
        row = cell >> (cols.bit_length() - 1)
        col = cell & (cols - 1)
        j = col >> (LANES.bit_length() - 1)
        shift = (k - col) & (LANES - 1)
        out = []
        mine = lane8 == k
        for q, hist in enumerate((he, hu, hv)):
            for h in range(groups):
                tile = hist[j, pl.ds((size * h + 1) * pitch + margin + row, size, stride=pitch), :]
                turned = pltpu.roll(tile, shift, 1)
                out.append(jnp.where(mine, turned, kept[q * groups + h]))
        return tuple(out)

    zero = jnp.zeros((size, LANES), jnp.float32)
    kept = lax.fori_loop(0, count, one_slot, (zero,) * (3 * groups), unroll=128)
    for t, tile in enumerate(kept):
        out_rec[size * t : size * (t + 1), :] = tile * (1.0 / DT) if t < groups else tile
    out_rec[3 * steps : 3 * steps + 8, :] = jnp.broadcast_to(ids[...].astype(jnp.float32), (8, LANES))


def place_kernel(base, rec, out, *, series, members):
    sources, _, slots = rec.shape
    gauges = members * GAUGE_DEV
    records = jnp.concatenate([rec[k, :series, :] for k in range(sources)], axis=1)
    one = records.astype(jnp.bfloat16)
    rest = records - one.astype(jnp.float32)
    two = rest.astype(jnp.bfloat16)
    three = (rest - two.astype(jnp.float32)).astype(jnp.bfloat16)
    terms = jnp.concatenate([one, two, three], axis=0)
    number = lax.broadcasted_iota(jnp.int32, (gauges, slots), 0)
    wanted = base[0] + (number // GAUGE_DEV) * (sources * GAUGE_DEV) + number % GAUGE_DEV
    wanted = wanted.astype(jnp.float32)
    picks = [
        (rec[k, series : series + 1, :] == wanted).astype(jnp.float32).astype(jnp.bfloat16)
        for k in range(sources)
    ]
    pick = jnp.concatenate(picks, axis=1)
    full = lax.dot_general(terms, pick, (((1,), (1,)), ((), ())), preferred_element_type=jnp.float32)
    dense = full[:series] + full[series : 2 * series] + full[2 * series :]
    half = series // 2
    low = lane_ids((half, LANES)) < GAUGE_DEV
    for t in range(gauges // LANES):
        tile = dense[:, LANES * t : LANES * (t + 1)]
        turned = pltpu.roll(tile, GAUGE_DEV, 1)
        out[2 * t] = jnp.where(low, tile[:half], turned[half:])
        out[2 * t + 1] = jnp.where(low, turned[:half], tile[half:])


def finish_kernel(parts, out, *, series):
    total = parts[0]
    for k in range(1, parts.shape[0]):
        total = total + parts[k]
    turned = pltpu.roll(total, GAUGE_DEV, 1)
    out[: series // 2, :] = total[:, :GAUGE_DEV]
    out[series // 2 :, :] = turned[:, :GAUGE_DEV]


def in_vmem(count):
    return [pl.BlockSpec(memory_space=pltpu.VMEM)] * count


def in_smem(count):
    return [pl.BlockSpec(memory_space=pltpu.SMEM)] * count


def f32(*shape):
    return jax.ShapeDtypeStruct(shape, jnp.float32)


def shards(surface, east, north, east_depth, north_depth, slot_gauge, slot_cell):
    rows, cols = surface.shape
    margin = STEPS
    series = 3 * STEPS
    n_gx, n_gy = lax.axis_size("gx"), lax.axis_size("gy")
    a, b = lax.axis_index("gx"), lax.axis_index("gy")
    fields = (surface, east, north, east_depth, north_depth)

    def shifted(tail, head, axis, count):
        from_before = lax.ppermute(tail, axis, [(i, i + 1) for i in range(count - 1)])
        from_after = lax.ppermute(head, axis, [(i + 1, i) for i in range(count - 1)])
        return from_before, from_after

    whole = pl.BlockSpec(memory_space=pltpu.HBM)
    head_rows, tail_rows = pl.pallas_call(
        functools.partial(pack_rows_kernel, margin=margin),
        out_shape=(f32(5 * margin, cols), f32(5 * margin, cols)),
        in_specs=[whole] * 5,
        out_specs=tuple(in_vmem(2)),
        scratch_shapes=[pltpu.SemaphoreType.DMA((10,))],
        compiler_params=pltpu.CompilerParams(vmem_limit_bytes=4 * MIB),
        name="pack_rows",
    )(*(pltpu.with_memory_space_constraint(f, pltpu.HBM) for f in fields))
    top, bot = shifted(tail_rows, head_rows, "gx", n_gx)

    height = rows + 2 * margin
    head, tail = pl.pallas_call(
        functools.partial(pack_columns_kernel, margin=margin),
        out_shape=(f32(height, LANES), f32(height, LANES)),
        in_specs=in_vmem(7),
        out_specs=tuple(in_vmem(2)),
        compiler_params=pltpu.CompilerParams(vmem_limit_bytes=4 * MIB),
        name="pack_columns",
    )(*fields, top, bot)
    from_left, from_right = shifted(tail, head, "gy", n_gy)

    tiles = cols // LANES + 1
    pitch = height + 8
    history = pltpu.VMEM((tiles, (STEPS + 1) * pitch, LANES), jnp.float32)
    depth = pltpu.VMEM((tiles, height, LANES), jnp.float32)
    eta, u, v, rec = pl.pallas_call(
        functools.partial(steps_kernel, steps=STEPS, last_x=n_gx - 1, last_y=n_gy - 1),
        out_shape=(pltpu.VMEM((rows, cols), jnp.float32),) * 3 + (f32(series + 8, LANES),),
        in_specs=[whole] + in_smem(2) + [whole] + in_vmem(9),
        out_specs=tuple(in_vmem(4)),
        scratch_shapes=[
            history, history, history, depth, depth,
            pltpu.SMEM(slot_cell.shape, jnp.int32),
            pltpu.VMEM(slot_gauge.shape, jnp.int32),
            pltpu.SemaphoreType.DMA((2,)),
        ],
        compiler_params=pltpu.CompilerParams(vmem_limit_bytes=24 * MIB),
        name="leapfrog",
    )(
        pltpu.with_memory_space_constraint(slot_cell, pltpu.HBM),
        a.astype(jnp.int32).reshape(1),
        b.astype(jnp.int32).reshape(1),
        pltpu.with_memory_space_constraint(slot_gauge, pltpu.HBM),
        *fields, top, bot, from_left, from_right,
    )

    near = [[QUAD * i + j for j in range(QUAD)] for i in range(n_gy // QUAD)]
    members = n_gy // QUAD
    far = [[i + QUAD * j for j in range(members)] for i in range(QUAD)]
    gathered = lax.all_gather(rec, "gy", axis_index_groups=near)
    base = (a * (n_gy * GAUGE_DEV) + (b % QUAD) * GAUGE_DEV).astype(jnp.int32).reshape(1)
    half = series // 2
    placed = pl.pallas_call(
        functools.partial(place_kernel, series=series, members=members),
        out_shape=f32(members, half, LANES),
        in_specs=in_smem(1) + in_vmem(1),
        out_specs=in_vmem(1)[0],
        compiler_params=pltpu.CompilerParams(vmem_limit_bytes=8 * MIB),
        name="place",
    )(base, gathered)
    arrived = lax.all_to_all(placed, "gy", 0, 0, axis_index_groups=far, tiled=True)
    out = pl.pallas_call(
        functools.partial(finish_kernel, series=series),
        out_shape=f32(series, GAUGE_DEV),
        in_specs=in_vmem(1),
        out_specs=in_vmem(1)[0],
        compiler_params=pltpu.CompilerParams(vmem_limit_bytes=4 * MIB),
        name="finish",
    )(arrived)
    return eta, u, v, out.T


def solution(mesh):
    block = P("gx", "gy")
    rows = P(("gx", "gy"), None)
    return jax.shard_map(
        shards,
        mesh=mesh,
        in_specs=(block,) * 5 + (rows, rows),
        out_specs=(block,) * 3 + (rows,),
        check_vma=False,
    )
```

```python
import functools

import jax
import jax.numpy as jnp
from jax import lax
from jax.experimental import pallas as pl
from jax.experimental.pallas import tpu as pltpu
from jax.sharding import PartitionSpec as P

STEPS = 16
GAUGE_DEV = 64
LANES = 128
DT = 0.45
MIB = 1 << 20


def lane_ids(shape):
    return lax.broadcasted_iota(jnp.int32, shape, 1)


def pack_columns_kernel(place_y, e, u, v, dx, dy, top, bot, near, far, *, margin):
    even = place_y[0] % 2 == 0
    rows, cols = e.shape
    lane = lane_ids((margin, LANES))
    last = cols - LANES
    fields = (e, u, v, dx, dy)
    for r in range(0, rows + 2 * margin, margin):
        out_head = jnp.zeros((margin, LANES), jnp.float32)
        out_tail = jnp.zeros((margin, LANES), jnp.float32)
        for f, ref in enumerate(fields):
            if r == 0:
                src, at = top, f * margin
            elif r == rows + margin:
                src, at = bot, f * margin
            else:
                src, at = ref, r - margin
            first = src[at : at + margin, :LANES]
            final = src[at : at + margin, last:]
            mine = (lane >= margin * f) & (lane < margin * (f + 1))
            if f:
                first = pltpu.roll(first, margin * f, 1)
            final = pltpu.roll(final, (margin * f + margin) % LANES, 1)
            out_head = jnp.where(mine, first, out_head)
            out_tail = jnp.where(mine, final, out_tail)
        near[r : r + margin, :] = jnp.where(even, out_tail, out_head)
        far[r : r + margin, :] = jnp.where(even, out_head, out_tail)


def pack_rows_kernel(e, u, v, dx, dy, head, tail, sems, *, margin):
    rows = e.shape[0]
    copies = []
    for f, ref in enumerate((e, u, v, dx, dy)):
        place = pl.ds(margin * f, margin)
        copies.append(pltpu.make_async_copy(ref.at[pl.ds(0, margin), :], head.at[place, :], sems.at[f]))
        copies.append(
            pltpu.make_async_copy(ref.at[pl.ds(rows - margin, margin), :], tail.at[place, :], sems.at[5 + f])
        )
    for copy in copies:
        copy.start()
    for copy in copies:
        copy.wait()


def steps_kernel(
    cells_in, place_x, place_y, ids_in, e, u, v, dx, dy, top, bot, from_near, from_far,
    out_e, out_u, out_v, out_rec, he, hu, hv, sx, sy, cells, ids, staged, list_sems, out_sems,
    *, steps, last_x, last_y,
):
    rows, cols = e.shape
    margin = steps
    own = cols // LANES
    tiles = own + 1
    height = rows + 2 * margin
    pitch = height + 8
    chunk = 16
    lane = lane_ids((chunk, LANES))
    even = place_y[0] % 2 == 0
    lists = [
        pltpu.make_async_copy(cells_in, cells, list_sems.at[0]),
        pltpu.make_async_copy(ids_in, ids, list_sems.at[1]),
    ]
    for copy in lists:
        copy.start()

    for f, (ref, dst, factor) in enumerate(
        ((e, he, DT), (u, hu, None), (v, hv, None), (dx, sx, DT * DT), (dy, sy, DT * DT))
    ):
        def scaled(value):
            return value if factor is None else value * factor

        for j in range(own):
            cut = slice(LANES * j, LANES * (j + 1))
            dst[j, :margin, :] = scaled(top[f * margin : (f + 1) * margin, cut])
            dst[j, margin : margin + rows, :] = scaled(ref[:, cut])
            dst[j, margin + rows : height, :] = scaled(bot[f * margin : (f + 1) * margin, cut])
        for r in range(0, height, chunk):
            crossed = from_far[r : r + chunk, :]
            right = jnp.where(even, from_near[1, r : r + chunk, :], crossed)
            left = jnp.where(even, crossed, from_near[0, r : r + chunk, :])
            if f:
                right = pltpu.roll(right, LANES - margin * f, 1)
            left = pltpu.roll(left, (LANES - margin - margin * f) % LANES, 1)
            tile = jnp.where(
                lane < margin, right, jnp.where(lane >= LANES - margin, left, jnp.zeros_like(left))
            )
            dst[own, r : r + chunk, :] = scaled(tile)

    size = 8
    lane8 = lane_ids((size, LANES))
    row8 = lax.broadcasted_iota(jnp.int32, (size, LANES), 0)
    first_lane, final_lane, final_row = lane8 == 0, lane8 == LANES - 1, row8 == size - 1
    keep_rows = place_x[0] != last_x
    keep_cols = (lane8 >= LANES // 2) | (place_y[0] != last_y)

    def one_step(low, s):
        now = pl.multiple_of(s * pitch, 8)
        new = pl.multiple_of(now + pitch, 8)
        flux_before = [None] * tiles
        for r in range(low, height - low, size):
            eta = [he[j, pl.ds(now + r, size), :] for j in range(tiles)]
            flux_y = []
            for j in range(tiles):
                right = pltpu.roll(jnp.where(first_lane, eta[(j + 1) % tiles], eta[j]), LANES - 1, 1)
                north = hv[j, pl.ds(now + r, size), :] - (right - eta[j])
                hv[j, pl.ds(new + r, size), :] = north
                flux_y.append(sy[j, r : r + size, :] * north)
            for j in range(tiles):
                down = he[j, pl.ds(now + r + 1, size), :]
                east = hu[j, pl.ds(now + r, size), :] - (down - eta[j])
                hu[j, pl.ds(new + r, size), :] = east
                flux_x = sx[j, r : r + size, :] * east
                above = flux_x if flux_before[j] is None else flux_before[j]
                flux_up = pltpu.roll(jnp.where(final_row, above, flux_x), 1, 0)
                flux_before[j] = flux_x
                flux_left = pltpu.roll(jnp.where(final_lane, flux_y[(j - 1) % tiles], flux_y[j]), 1, 1)
                after = eta[j] - ((flux_x - flux_up) + (flux_y[j] - flux_left))
                if j == own:
                    after = jnp.where(keep_cols, after, 0.0)
                if r >= rows + margin:
                    after = jnp.where(keep_rows, after, 0.0)
                he[j, pl.ds(new + r, size), :] = after

    for low in range(0, steps, size):
        lax.fori_loop(low, low + size, lambda s, _: one_step(low, s), None, unroll=1)

    last = steps * pitch + margin
    outs = []
    for j in range(own):
        cut = pl.ds(LANES * j, LANES)
        outs.append(pltpu.make_async_copy(hu.at[j, pl.ds(last, rows), :], out_u.at[:, cut], out_sems.at[j]))
        outs.append(
            pltpu.make_async_copy(hv.at[j, pl.ds(last, rows), :], out_v.at[:, cut], out_sems.at[own + j])
        )
    outs.append(pltpu.make_async_copy(staged, out_e, out_sems.at[2 * own]))
    for copy in outs[:-1]:
        copy.start()
    for j in range(own):
        staged[:, LANES * j : LANES * (j + 1)] = he[j, last : last + rows, :] * (1.0 / DT)
    outs[-1].start()
    for copy in lists:
        copy.wait()

    count = cells.shape[1]
    groups = steps // size

    def one_slot(k, kept):
        cell = cells[0, k]
        row = cell >> (cols.bit_length() - 1)
        col = cell & (cols - 1)
        j = col >> (LANES.bit_length() - 1)
        shift = (k - col) & (LANES - 1)
        out = []
        mine = lane8 == k
        for q, hist in enumerate((he, hu, hv)):
            for h in range(groups):
                tile = hist[j, pl.ds((size * h + 1) * pitch + margin + row, size, stride=pitch), :]
                turned = pltpu.roll(tile, shift, 1)
                out.append(jnp.where(mine, turned, kept[q * groups + h]))
        return tuple(out)

    zero = jnp.zeros((size, LANES), jnp.float32)
    kept = lax.fori_loop(0, count, one_slot, (zero,) * (3 * groups), unroll=128)
    for t, tile in enumerate(kept):
        out_rec[size * t : size * (t + 1), :] = tile * (1.0 / DT) if t < groups else tile
    out_rec[3 * steps : 3 * steps + 8, :] = jnp.broadcast_to(ids[...].astype(jnp.float32), (8, LANES))
    for copy in outs:
        copy.wait()


def place_kernel(base, rec, out, *, series, members):
    sources, _, slots = rec.shape
    gauges = members * GAUGE_DEV
    records = jnp.concatenate([rec[k, :series, :] for k in range(sources)], axis=1)
    one = records.astype(jnp.bfloat16)
    rest = records - one.astype(jnp.float32)
    two = rest.astype(jnp.bfloat16)
    three = (rest - two.astype(jnp.float32)).astype(jnp.bfloat16)
    terms = jnp.concatenate([one, two, three], axis=0)
    number = lax.broadcasted_iota(jnp.int32, (gauges, slots), 0)
    wanted = base[0] + (number // GAUGE_DEV) * (sources * GAUGE_DEV) + number % GAUGE_DEV
    wanted = wanted.astype(jnp.float32)
    picks = [
        (rec[k, series : series + 1, :] == wanted).astype(jnp.float32).astype(jnp.bfloat16)
        for k in range(sources)
    ]
    pick = jnp.concatenate(picks, axis=1)
    full = lax.dot_general(terms, pick, (((1,), (1,)), ((), ())), preferred_element_type=jnp.float32)
    dense = full[:series] + full[series : 2 * series] + full[2 * series :]
    half = series // 2
    low = lane_ids((half, LANES)) < GAUGE_DEV
    for t in range(gauges // LANES):
        tile = dense[:, LANES * t : LANES * (t + 1)]
        turned = pltpu.roll(tile, GAUGE_DEV, 1)
        out[2 * t] = jnp.where(low, tile[:half], turned[half:])
        out[2 * t + 1] = jnp.where(low, turned[:half], tile[half:])


def finish_kernel(parts, out, *, series):
    total = parts[0]
    for k in range(1, parts.shape[0]):
        total = total + parts[k]
    turned = pltpu.roll(total, GAUGE_DEV, 1)
    out[: series // 2, :] = total[:, :GAUGE_DEV]
    out[series // 2 :, :] = turned[:, :GAUGE_DEV]


def in_vmem(count):
    return [pl.BlockSpec(memory_space=pltpu.VMEM)] * count


def in_smem(count):
    return [pl.BlockSpec(memory_space=pltpu.SMEM)] * count


def f32(*shape):
    return jax.ShapeDtypeStruct(shape, jnp.float32)


def shards(surface, east, north, east_depth, north_depth, slot_gauge, slot_cell):
    rows, cols = surface.shape
    margin = STEPS
    series = 3 * STEPS
    n_gx, n_gy = lax.axis_size("gx"), lax.axis_size("gy")
    a, b = lax.axis_index("gx"), lax.axis_index("gy")
    fields = (surface, east, north, east_depth, north_depth)

    whole = pl.BlockSpec(memory_space=pltpu.HBM)
    head_rows, tail_rows = pl.pallas_call(
        functools.partial(pack_rows_kernel, margin=margin),
        out_shape=(f32(5 * margin, cols), f32(5 * margin, cols)),
        in_specs=[whole] * 5,
        out_specs=tuple(in_vmem(2)),
        scratch_shapes=[pltpu.SemaphoreType.DMA((10,))],
        compiler_params=pltpu.CompilerParams(vmem_limit_bytes=4 * MIB),
        name="pack_rows",
    )(*(pltpu.with_memory_space_constraint(f, pltpu.HBM) for f in fields))
    top = lax.ppermute(tail_rows, "gx", [(i, i + 1) for i in range(n_gx - 1)])
    bot = lax.ppermute(head_rows, "gx", [(i + 1, i) for i in range(n_gx - 1)])

    height = rows + 2 * margin
    place_x = a.astype(jnp.int32).reshape(1)
    place_y = b.astype(jnp.int32).reshape(1)
    near, far = pl.pallas_call(
        functools.partial(pack_columns_kernel, margin=margin),
        out_shape=(f32(height, LANES), f32(height, LANES)),
        in_specs=in_smem(1) + in_vmem(7),
        out_specs=tuple(in_vmem(2)),
        compiler_params=pltpu.CompilerParams(vmem_limit_bytes=4 * MIB),
        name="pack_columns",
    )(place_y, *fields, top, bot)
    bonds = [(i, i + 1) for i in range(1, n_gy - 1, 2)]
    pairs = [[2 * i, 2 * i + 1] for i in range(n_gy // 2)]
    from_far = lax.ppermute(far, "gy", bonds + [(j, i) for i, j in bonds])
    from_near = lax.all_gather(near, "gy", axis_index_groups=pairs)

    tiles = cols // LANES + 1
    pitch = height + 8
    history = pltpu.VMEM((tiles, (STEPS + 1) * pitch, LANES), jnp.float32)
    depth = pltpu.VMEM((tiles, height, LANES), jnp.float32)
    eta, u, v, rec = pl.pallas_call(
        functools.partial(steps_kernel, steps=STEPS, last_x=n_gx - 1, last_y=n_gy - 1),
        out_shape=(f32(rows, cols),) * 3 + (f32(series + 8, LANES),),
        in_specs=[whole] + in_smem(2) + [whole] + in_vmem(9),
        out_specs=(whole,) * 3 + tuple(in_vmem(1)),
        scratch_shapes=[
            history, history, history, depth, depth,
            pltpu.SMEM(slot_cell.shape, jnp.int32),
            pltpu.VMEM(slot_gauge.shape, jnp.int32),
            pltpu.VMEM((rows, cols), jnp.float32),
            pltpu.SemaphoreType.DMA((2,)),
            pltpu.SemaphoreType.DMA((2 * tiles - 1,)),
        ],
        compiler_params=pltpu.CompilerParams(vmem_limit_bytes=24 * MIB),
        name="leapfrog",
    )(
        pltpu.with_memory_space_constraint(slot_cell, pltpu.HBM),
        place_x,
        place_y,
        pltpu.with_memory_space_constraint(slot_gauge, pltpu.HBM),
        *fields, top, bot, from_near, from_far,
    )

    members = n_gy // 2
    chips = [[i + 2 * j for j in range(members)] for i in range(2)]
    gathered = lax.all_gather(rec, "gy", axis_index_groups=pairs)
    base = (a * (n_gy * GAUGE_DEV) + (b % 2) * GAUGE_DEV).astype(jnp.int32).reshape(1)
    half = series // 2
    placed = pl.pallas_call(
        functools.partial(place_kernel, series=series, members=members),
        out_shape=f32(members, half, LANES),
        in_specs=in_smem(1) + in_vmem(1),
        out_specs=in_vmem(1)[0],
        compiler_params=pltpu.CompilerParams(vmem_limit_bytes=8 * MIB),
        name="place",
    )(base, gathered)
    arrived = lax.all_to_all(placed, "gy", 0, 0, axis_index_groups=chips, tiled=True)
    out = pl.pallas_call(
        functools.partial(finish_kernel, series=series),
        out_shape=f32(series, GAUGE_DEV),
        in_specs=in_vmem(1),
        out_specs=in_vmem(1)[0],
        compiler_params=pltpu.CompilerParams(vmem_limit_bytes=4 * MIB),
        name="finish",
    )(arrived)
    return eta, u, v, out.T


def solution(mesh):
    block = P("gx", "gy")
    rows = P(("gx", "gy"), None)
    return jax.shard_map(
        shards,
        mesh=mesh,
        in_specs=(block,) * 5 + (rows, rows),
        out_specs=(block,) * 3 + (rows,),
        check_vma=False,
    )
```

```python
import functools

import jax
import jax.numpy as jnp
from jax import lax
from jax.experimental import pallas as pl
from jax.experimental.pallas import tpu as pltpu
from jax.sharding import PartitionSpec as P

STEPS = 16
GAUGE_DEV = 64
LANES = 128
DT = 0.45
MIB = 1 << 20


def lane_ids(shape):
    return lax.broadcasted_iota(jnp.int32, shape, 1)


def pack_columns_kernel(place_x, place_y, e, u, v, dx, dy, row_near, row_far, near, far, *, margin):
    even = place_y[0] % 2 == 0
    even_x = place_x[0] % 2 == 0
    rows, cols = e.shape
    lane = lane_ids((margin, LANES))
    last = cols - LANES
    fields = (e, u, v, dx, dy)
    for r in range(0, rows + 2 * margin, margin):
        out_head = jnp.zeros((margin, LANES), jnp.float32)
        out_tail = jnp.zeros((margin, LANES), jnp.float32)
        for f, ref in enumerate(fields):
            halo = slice(f * margin, (f + 1) * margin)

            def piece(cut):
                if r == 0:
                    return jnp.where(even_x, row_far[halo, cut], row_near[0, halo, cut])
                if r == rows + margin:
                    return jnp.where(even_x, row_near[1, halo, cut], row_far[halo, cut])
                return ref[r - margin : r, cut]

            first = piece(slice(0, LANES))
            final = piece(slice(last, last + LANES))
            mine = (lane >= margin * f) & (lane < margin * (f + 1))
            if f:
                first = pltpu.roll(first, margin * f, 1)
            final = pltpu.roll(final, (margin * f + margin) % LANES, 1)
            out_head = jnp.where(mine, first, out_head)
            out_tail = jnp.where(mine, final, out_tail)
        near[r : r + margin, :] = jnp.where(even, out_tail, out_head)
        far[r : r + margin, :] = jnp.where(even, out_head, out_tail)


def pack_rows_kernel(place_x, e, u, v, dx, dy, near, far, sems, *, margin):
    last = e.shape[0] - margin
    even = place_x[0] % 2 == 0
    near_from = pl.multiple_of(jnp.where(even, last, 0), margin)
    far_from = pl.multiple_of(jnp.where(even, 0, last), margin)
    copies = []
    for f, ref in enumerate((e, u, v, dx, dy)):
        place = pl.ds(margin * f, margin)
        copies.append(
            pltpu.make_async_copy(ref.at[pl.ds(near_from, margin), :], near.at[place, :], sems.at[f])
        )
        copies.append(
            pltpu.make_async_copy(ref.at[pl.ds(far_from, margin), :], far.at[place, :], sems.at[5 + f])
        )
    for copy in copies:
        copy.start()
    for copy in copies:
        copy.wait()


def steps_kernel(
    cells_in, place_x, place_y, ids_in, e, u, v, dx, dy, row_near, row_far, from_near, from_far,
    out_e, out_u, out_v, out_rec, he, hu, hv, sx, sy, cells, ids, staged, list_sems, out_sems,
    *, steps, last_x, last_y,
):
    rows, cols = e.shape
    margin = steps
    own = cols // LANES
    tiles = own + 1
    height = rows + 2 * margin
    pitch = height + 8
    chunk = 16
    lane = lane_ids((chunk, LANES))
    even = place_y[0] % 2 == 0
    even_x = place_x[0] % 2 == 0
    lists = [
        pltpu.make_async_copy(cells_in, cells, list_sems.at[0]),
        pltpu.make_async_copy(ids_in, ids, list_sems.at[1]),
    ]
    for copy in lists:
        copy.start()

    for f, (ref, dst, factor) in enumerate(
        ((e, he, DT), (u, hu, None), (v, hv, None), (dx, sx, DT * DT), (dy, sy, DT * DT))
    ):
        def scaled(value):
            return value if factor is None else value * factor

        for j in range(own):
            cut = slice(LANES * j, LANES * (j + 1))
            halo = slice(f * margin, (f + 1) * margin)
            crossed = row_far[halo, cut]
            dst[j, :margin, :] = scaled(jnp.where(even_x, crossed, row_near[0, halo, cut]))
            dst[j, margin : margin + rows, :] = scaled(ref[:, cut])
            dst[j, margin + rows : height, :] = scaled(jnp.where(even_x, row_near[1, halo, cut], crossed))
        for r in range(0, height, chunk):
            crossed = from_far[r : r + chunk, :]
            right = jnp.where(even, from_near[1, r : r + chunk, :], crossed)
            left = jnp.where(even, crossed, from_near[0, r : r + chunk, :])
            if f:
                right = pltpu.roll(right, LANES - margin * f, 1)
            left = pltpu.roll(left, (LANES - margin - margin * f) % LANES, 1)
            tile = jnp.where(
                lane < margin, right, jnp.where(lane >= LANES - margin, left, jnp.zeros_like(left))
            )
            dst[own, r : r + chunk, :] = scaled(tile)

    size = 8
    lane8 = lane_ids((size, LANES))
    row8 = lax.broadcasted_iota(jnp.int32, (size, LANES), 0)
    first_lane, final_lane, final_row = lane8 == 0, lane8 == LANES - 1, row8 == size - 1
    keep_rows = place_x[0] != last_x
    keep_cols = (lane8 >= LANES // 2) | (place_y[0] != last_y)

    def one_step(low, s):
        now = pl.multiple_of(s * pitch, 8)
        new = pl.multiple_of(now + pitch, 8)
        flux_before = [None] * tiles
        for r in range(low, height - low, size):
            eta = [he[j, pl.ds(now + r, size), :] for j in range(tiles)]
            flux_y = []
            for j in range(tiles):
                right = pltpu.roll(jnp.where(first_lane, eta[(j + 1) % tiles], eta[j]), LANES - 1, 1)
                north = hv[j, pl.ds(now + r, size), :] - (right - eta[j])
                hv[j, pl.ds(new + r, size), :] = north
                flux_y.append(sy[j, r : r + size, :] * north)
            for j in range(tiles):
                down = he[j, pl.ds(now + r + 1, size), :]
                east = hu[j, pl.ds(now + r, size), :] - (down - eta[j])
                hu[j, pl.ds(new + r, size), :] = east
                flux_x = sx[j, r : r + size, :] * east
                above = flux_x if flux_before[j] is None else flux_before[j]
                flux_up = pltpu.roll(jnp.where(final_row, above, flux_x), 1, 0)
                flux_before[j] = flux_x
                flux_left = pltpu.roll(jnp.where(final_lane, flux_y[(j - 1) % tiles], flux_y[j]), 1, 1)
                after = eta[j] - ((flux_x - flux_up) + (flux_y[j] - flux_left))
                if j == own:
                    after = jnp.where(keep_cols, after, 0.0)
                if r >= rows + margin:
                    after = jnp.where(keep_rows, after, 0.0)
                he[j, pl.ds(new + r, size), :] = after

    for low in range(0, steps, size):
        lax.fori_loop(low, low + size, lambda s, _: one_step(low, s), None, unroll=1)

    last = steps * pitch + margin
    outs = []
    for j in range(own):
        cut = pl.ds(LANES * j, LANES)
        outs.append(pltpu.make_async_copy(hu.at[j, pl.ds(last, rows), :], out_u.at[:, cut], out_sems.at[j]))
        outs.append(
            pltpu.make_async_copy(hv.at[j, pl.ds(last, rows), :], out_v.at[:, cut], out_sems.at[own + j])
        )
    outs.append(pltpu.make_async_copy(staged, out_e, out_sems.at[2 * own]))
    for copy in outs[:-1]:
        copy.start()
    for j in range(own):
        staged[:, LANES * j : LANES * (j + 1)] = he[j, last : last + rows, :] * (1.0 / DT)
    outs[-1].start()
    for copy in lists:
        copy.wait()

    count = cells.shape[1]
    groups = steps // size

    def one_slot(k, kept):
        cell = cells[0, k]
        row = cell >> (cols.bit_length() - 1)
        col = cell & (cols - 1)
        j = col >> (LANES.bit_length() - 1)
        shift = (k - col) & (LANES - 1)
        out = []
        mine = lane8 == k
        for q, hist in enumerate((he, hu, hv)):
            for h in range(groups):
                tile = hist[j, pl.ds((size * h + 1) * pitch + margin + row, size, stride=pitch), :]
                turned = pltpu.roll(tile, shift, 1)
                out.append(jnp.where(mine, turned, kept[q * groups + h]))
        return tuple(out)

    zero = jnp.zeros((size, LANES), jnp.float32)
    kept = lax.fori_loop(0, count, one_slot, (zero,) * (3 * groups), unroll=128)
    for t, tile in enumerate(kept):
        out_rec[size * t : size * (t + 1), :] = tile * (1.0 / DT) if t < groups else tile
    out_rec[3 * steps : 3 * steps + 8, :] = jnp.broadcast_to(ids[...].astype(jnp.float32), (8, LANES))
    for copy in outs:
        copy.wait()


def place_kernel(base, rec, out, *, series, members):
    sources, _, slots = rec.shape
    gauges = members * GAUGE_DEV
    records = jnp.concatenate([rec[k, :series, :] for k in range(sources)], axis=1)
    one = records.astype(jnp.bfloat16)
    rest = records - one.astype(jnp.float32)
    two = rest.astype(jnp.bfloat16)
    three = (rest - two.astype(jnp.float32)).astype(jnp.bfloat16)
    terms = jnp.concatenate([one, two, three], axis=0)
    number = lax.broadcasted_iota(jnp.int32, (gauges, slots), 0)
    wanted = base[0] + (number // GAUGE_DEV) * (sources * GAUGE_DEV) + number % GAUGE_DEV
    wanted = wanted.astype(jnp.float32)
    picks = [
        (rec[k, series : series + 1, :] == wanted).astype(jnp.float32).astype(jnp.bfloat16)
        for k in range(sources)
    ]
    pick = jnp.concatenate(picks, axis=1)
    full = lax.dot_general(terms, pick, (((1,), (1,)), ((), ())), preferred_element_type=jnp.float32)
    dense = full[:series] + full[series : 2 * series] + full[2 * series :]
    half = series // 2
    low = lane_ids((half, LANES)) < GAUGE_DEV
    for t in range(gauges // LANES):
        tile = dense[:, LANES * t : LANES * (t + 1)]
        turned = pltpu.roll(tile, GAUGE_DEV, 1)
        out[2 * t] = jnp.where(low, tile[:half], turned[half:])
        out[2 * t + 1] = jnp.where(low, turned[:half], tile[half:])


def finish_kernel(parts, out, *, series):
    total = parts[0]
    for k in range(1, parts.shape[0]):
        total = total + parts[k]
    turned = pltpu.roll(total, GAUGE_DEV, 1)
    out[: series // 2, :] = total[:, :GAUGE_DEV]
    out[series // 2 :, :] = turned[:, :GAUGE_DEV]


def in_vmem(count):
    return [pl.BlockSpec(memory_space=pltpu.VMEM)] * count


def in_smem(count):
    return [pl.BlockSpec(memory_space=pltpu.SMEM)] * count


def f32(*shape):
    return jax.ShapeDtypeStruct(shape, jnp.float32)


def shards(surface, east, north, east_depth, north_depth, slot_gauge, slot_cell):
    rows, cols = surface.shape
    margin = STEPS
    series = 3 * STEPS
    n_gx, n_gy = lax.axis_size("gx"), lax.axis_size("gy")
    a, b = lax.axis_index("gx"), lax.axis_index("gy")
    fields = (surface, east, north, east_depth, north_depth)

    whole = pl.BlockSpec(memory_space=pltpu.HBM)
    place_x = a.astype(jnp.int32).reshape(1)
    place_y = b.astype(jnp.int32).reshape(1)

    def bonds(count):
        links = [(i, i + 1) for i in range(1, count - 1, 2)]
        return links + [(j, i) for i, j in links]

    def pairs(count):
        return [[2 * i, 2 * i + 1] for i in range(count // 2)]

    near, far = pl.pallas_call(
        functools.partial(pack_rows_kernel, margin=margin),
        out_shape=(f32(5 * margin, cols), f32(5 * margin, cols)),
        in_specs=in_smem(1) + [whole] * 5,
        out_specs=tuple(in_vmem(2)),
        scratch_shapes=[pltpu.SemaphoreType.DMA((10,))],
        compiler_params=pltpu.CompilerParams(vmem_limit_bytes=4 * MIB),
        name="pack_rows",
    )(place_x, *(pltpu.with_memory_space_constraint(f, pltpu.HBM) for f in fields))
    row_far = lax.ppermute(far, "gx", bonds(n_gx))
    row_near = lax.all_gather(near, "gx", axis_index_groups=pairs(n_gx))

    height = rows + 2 * margin
    near, far = pl.pallas_call(
        functools.partial(pack_columns_kernel, margin=margin),
        out_shape=(f32(height, LANES), f32(height, LANES)),
        in_specs=in_smem(2) + in_vmem(7),
        out_specs=tuple(in_vmem(2)),
        compiler_params=pltpu.CompilerParams(vmem_limit_bytes=4 * MIB),
        name="pack_columns",
    )(place_x, place_y, *fields, row_near, row_far)
    from_far = lax.ppermute(far, "gy", bonds(n_gy))
    from_near = lax.all_gather(near, "gy", axis_index_groups=pairs(n_gy))

    tiles = cols // LANES + 1
    pitch = height + 8
    history = pltpu.VMEM((tiles, (STEPS + 1) * pitch, LANES), jnp.float32)
    depth = pltpu.VMEM((tiles, height, LANES), jnp.float32)
    eta, u, v, rec = pl.pallas_call(
        functools.partial(steps_kernel, steps=STEPS, last_x=n_gx - 1, last_y=n_gy - 1),
        out_shape=(f32(rows, cols),) * 3 + (f32(series + 8, LANES),),
        in_specs=[whole] + in_smem(2) + [whole] + in_vmem(9),
        out_specs=(whole,) * 3 + tuple(in_vmem(1)),
        scratch_shapes=[
            history, history, history, depth, depth,
            pltpu.SMEM(slot_cell.shape, jnp.int32),
            pltpu.VMEM(slot_gauge.shape, jnp.int32),
            pltpu.VMEM((rows, cols), jnp.float32),
            pltpu.SemaphoreType.DMA((2,)),
            pltpu.SemaphoreType.DMA((2 * tiles - 1,)),
        ],
        compiler_params=pltpu.CompilerParams(
            vmem_limit_bytes=24 * MIB
        ),
        name="leapfrog",
    )(
        pltpu.with_memory_space_constraint(slot_cell, pltpu.HBM),
        place_x,
        place_y,
        pltpu.with_memory_space_constraint(slot_gauge, pltpu.HBM),
        *fields, row_near, row_far, from_near, from_far,
    )

    members = n_gy // 2
    chips = [[i + 2 * j for j in range(members)] for i in range(2)]
    gathered = lax.all_gather(rec, "gy", axis_index_groups=pairs(n_gy))
    base = (a * (n_gy * GAUGE_DEV) + (b % 2) * GAUGE_DEV).astype(jnp.int32).reshape(1)
    half = series // 2
    placed = pl.pallas_call(
        functools.partial(place_kernel, series=series, members=members),
        out_shape=f32(members, half, LANES),
        in_specs=in_smem(1) + in_vmem(1),
        out_specs=in_vmem(1)[0],
        compiler_params=pltpu.CompilerParams(vmem_limit_bytes=8 * MIB),
        name="place",
    )(base, gathered)
    arrived = lax.all_to_all(placed, "gy", 0, 0, axis_index_groups=chips, tiled=True)
    out = pl.pallas_call(
        functools.partial(finish_kernel, series=series),
        out_shape=f32(series, GAUGE_DEV),
        in_specs=in_vmem(1),
        out_specs=in_vmem(1)[0],
        compiler_params=pltpu.CompilerParams(vmem_limit_bytes=4 * MIB),
        name="finish",
    )(arrived)
    return eta, u, v, out.T


def solution(mesh):
    block = P("gx", "gy")
    rows = P(("gx", "gy"), None)
    return jax.shard_map(
        shards,
        mesh=mesh,
        in_specs=(block,) * 5 + (rows, rows),
        out_specs=(block,) * 3 + (rows,),
        check_vma=False,
    )
```

```python
import functools

import jax
import jax.numpy as jnp
from jax import lax
from jax.experimental import pallas as pl
from jax.experimental.pallas import tpu as pltpu
from jax.sharding import PartitionSpec as P

STEPS = 16
GAUGE_DEV = 64
LANES = 128
DT = 0.45
MIB = 1 << 20


def lane_ids(shape):
    return lax.broadcasted_iota(jnp.int32, shape, 1)


def pack_columns_kernel(place_x, place_y, e, u, v, dx, dy, row_near, row_far, near, far, *, margin):
    even = place_y[0] % 2 == 0
    even_x = place_x[0] % 2 == 0
    rows, cols = e.shape
    lane = lane_ids((margin, LANES))
    last = cols - LANES
    fields = (e, u, v, dx, dy)
    for r in range(0, rows + 2 * margin, margin):
        out_head = jnp.zeros((margin, LANES), jnp.float32)
        out_tail = jnp.zeros((margin, LANES), jnp.float32)
        for f, ref in enumerate(fields):
            halo = slice(f * margin, (f + 1) * margin)

            def piece(cut):
                if r == 0:
                    return jnp.where(even_x, row_far[halo, cut], row_near[0, halo, cut])
                if r == rows + margin:
                    return jnp.where(even_x, row_near[1, halo, cut], row_far[halo, cut])
                return ref[r - margin : r, cut]

            first = piece(slice(0, LANES))
            final = piece(slice(last, last + LANES))
            mine = (lane >= margin * f) & (lane < margin * (f + 1))
            if f:
                first = pltpu.roll(first, margin * f, 1)
            final = pltpu.roll(final, (margin * f + margin) % LANES, 1)
            out_head = jnp.where(mine, first, out_head)
            out_tail = jnp.where(mine, final, out_tail)
        near[r : r + margin, :] = jnp.where(even, out_tail, out_head)
        far[r : r + margin, :] = jnp.where(even, out_head, out_tail)


def pack_rows_kernel(place_x, e, u, v, dx, dy, near, far, sems, *, margin):
    last = e.shape[0] - margin
    even = place_x[0] % 2 == 0
    near_from = pl.multiple_of(jnp.where(even, last, 0), margin)
    far_from = pl.multiple_of(jnp.where(even, 0, last), margin)
    copies = []
    for f, ref in enumerate((e, u, v, dx, dy)):
        place = pl.ds(margin * f, margin)
        copies.append(
            pltpu.make_async_copy(ref.at[pl.ds(near_from, margin), :], near.at[place, :], sems.at[f])
        )
        copies.append(
            pltpu.make_async_copy(ref.at[pl.ds(far_from, margin), :], far.at[place, :], sems.at[5 + f])
        )
    for copy in copies:
        copy.start()
    for copy in copies:
        copy.wait()


def steps_kernel(
    cells_in, place_x, place_y, ids_in, e, u, v, dx, dy, row_near, row_far, from_near, from_far,
    out_e, out_u, out_v, out_rec, he, hu, hv, sx, sy, vl, syl, cells, ids, staged, list_sems, out_sems,
    *, steps, last_x, last_y,
):
    rows, cols = e.shape
    margin = steps
    own = cols // LANES
    tiles = own + 1
    height = rows + 2 * margin
    pitch = height + 8
    chunk = 16
    lane = lane_ids((chunk, LANES))
    even = place_y[0] % 2 == 0
    even_x = place_x[0] % 2 == 0
    lists = [
        pltpu.make_async_copy(cells_in, cells, list_sems.at[0]),
        pltpu.make_async_copy(ids_in, ids, list_sems.at[1]),
    ]
    for copy in lists:
        copy.start()

    for f, (ref, dst, factor) in enumerate(
        ((e, he, DT), (u, hu, None), (v, hv, None), (dx, sx, DT * DT), (dy, sy, DT * DT))
    ):
        def scaled(value):
            return value if factor is None else value * factor

        for j in range(own):
            cut = slice(LANES * j, LANES * (j + 1))
            halo = slice(f * margin, (f + 1) * margin)
            crossed = row_far[halo, cut]
            dst[j, :margin, :] = scaled(jnp.where(even_x, crossed, row_near[0, halo, cut]))
            dst[j, margin : margin + rows, :] = scaled(ref[:, cut])
            dst[j, margin + rows : height, :] = scaled(jnp.where(even_x, row_near[1, halo, cut], crossed))
        for r in range(0, height, chunk):
            crossed = from_far[r : r + chunk, :]
            right = jnp.where(even, from_near[1, r : r + chunk, :], crossed)
            left = jnp.where(even, crossed, from_near[0, r : r + chunk, :])
            if f:
                right = pltpu.roll(right, LANES - margin * f, 1)
            left = pltpu.roll(left, (LANES - margin - margin * f) % LANES, 1)
            tile = jnp.where(
                lane < margin, right, jnp.where(lane >= LANES - margin, left, jnp.zeros_like(left))
            )
            dst[own, r : r + chunk, :] = scaled(tile)

    size = 8
    lane8 = lane_ids((size, LANES))
    row8 = lax.broadcasted_iota(jnp.int32, (size, LANES), 0)
    first_lane, final_lane, final_row = lane8 == 0, lane8 == LANES - 1, row8 == size - 1
    keep_rows = place_x[0] != last_x
    keep_cols = (lane8 >= LANES // 2) | (place_y[0] != last_y)

    for src, dst in ((hv, vl), (sy, syl)):
        for r in range(0, height, size):
            tilesv = [src[j, r : r + size, :] for j in range(tiles)]
            for j in range(tiles):
                dst[j, r : r + size, :] = pltpu.roll(
                    jnp.where(final_lane, tilesv[(j - 1) % tiles], tilesv[j]), 1, 1
                )

    def one_step(low, s):
        now = pl.multiple_of(s * pitch, 8)
        new = pl.multiple_of(now + pitch, 8)
        flux_before = [None] * tiles
        for r in range(low, height - low, size):
            eta = [he[j, pl.ds(now + r, size), :] for j in range(tiles)]
            cross = []
            for j in range(tiles):
                right = pltpu.roll(jnp.where(first_lane, eta[(j + 1) % tiles], eta[j]), LANES - 1, 1)
                north = hv[j, pl.ds(now + r, size), :] - (right - eta[j])
                hv[j, pl.ds(new + r, size), :] = north
                left = pltpu.roll(jnp.where(final_lane, eta[(j - 1) % tiles], eta[j]), 1, 1)
                behind = vl[j, r : r + size, :] - (eta[j] - left)
                vl[j, r : r + size, :] = behind
                cross.append(sy[j, r : r + size, :] * north - syl[j, r : r + size, :] * behind)
            for j in range(tiles):
                down = he[j, pl.ds(now + r + 1, size), :]
                east = hu[j, pl.ds(now + r, size), :] - (down - eta[j])
                hu[j, pl.ds(new + r, size), :] = east
                flux_x = sx[j, r : r + size, :] * east
                above = flux_x if flux_before[j] is None else flux_before[j]
                flux_up = pltpu.roll(jnp.where(final_row, above, flux_x), 1, 0)
                flux_before[j] = flux_x
                after = eta[j] - ((flux_x - flux_up) + cross[j])
                if j == own:
                    after = jnp.where(keep_cols, after, 0.0)
                if r >= rows + margin:
                    after = jnp.where(keep_rows, after, 0.0)
                he[j, pl.ds(new + r, size), :] = after

    for low in range(0, steps, size):
        lax.fori_loop(low, low + size, lambda s, _: one_step(low, s), None, unroll=size)

    last = steps * pitch + margin
    outs = []
    for j in range(own):
        cut = pl.ds(LANES * j, LANES)
        outs.append(pltpu.make_async_copy(hu.at[j, pl.ds(last, rows), :], out_u.at[:, cut], out_sems.at[j]))
        outs.append(
            pltpu.make_async_copy(hv.at[j, pl.ds(last, rows), :], out_v.at[:, cut], out_sems.at[own + j])
        )
    outs.append(pltpu.make_async_copy(staged, out_e, out_sems.at[2 * own]))
    for copy in outs[:-1]:
        copy.start()
    for j in range(own):
        staged[:, LANES * j : LANES * (j + 1)] = he[j, last : last + rows, :] * (1.0 / DT)
    outs[-1].start()
    for copy in lists:
        copy.wait()

    count = cells.shape[1]
    groups = steps // size

    def one_slot(k, kept):
        cell = cells[0, k]
        row = cell >> (cols.bit_length() - 1)
        col = cell & (cols - 1)
        j = col >> (LANES.bit_length() - 1)
        shift = (k - col) & (LANES - 1)
        out = []
        mine = lane8 == k
        for q, hist in enumerate((he, hu, hv)):
            for h in range(groups):
                tile = hist[j, pl.ds((size * h + 1) * pitch + margin + row, size, stride=pitch), :]
                turned = pltpu.roll(tile, shift, 1)
                out.append(jnp.where(mine, turned, kept[q * groups + h]))
        return tuple(out)

    zero = jnp.zeros((size, LANES), jnp.float32)
    kept = lax.fori_loop(0, count, one_slot, (zero,) * (3 * groups), unroll=128)
    for t, tile in enumerate(kept):
        out_rec[size * t : size * (t + 1), :] = tile * (1.0 / DT) if t < groups else tile
    out_rec[3 * steps : 3 * steps + 8, :] = jnp.broadcast_to(ids[...].astype(jnp.float32), (8, LANES))
    for copy in outs:
        copy.wait()


def place_kernel(base, rec, out, *, series, members):
    sources, _, slots = rec.shape
    gauges = members * GAUGE_DEV
    records = jnp.concatenate([rec[k, :series, :] for k in range(sources)], axis=1)
    one = records.astype(jnp.bfloat16)
    rest = records - one.astype(jnp.float32)
    two = rest.astype(jnp.bfloat16)
    three = (rest - two.astype(jnp.float32)).astype(jnp.bfloat16)
    terms = jnp.concatenate([one, two, three], axis=0)
    number = lax.broadcasted_iota(jnp.int32, (gauges, slots), 0)
    wanted = base[0] + (number // GAUGE_DEV) * (sources * GAUGE_DEV) + number % GAUGE_DEV
    wanted = wanted.astype(jnp.float32)
    picks = [
        (rec[k, series : series + 1, :] == wanted).astype(jnp.float32).astype(jnp.bfloat16)
        for k in range(sources)
    ]
    pick = jnp.concatenate(picks, axis=1)
    full = lax.dot_general(terms, pick, (((1,), (1,)), ((), ())), preferred_element_type=jnp.float32)
    dense = full[:series] + full[series : 2 * series] + full[2 * series :]
    half = series // 2
    low = lane_ids((half, LANES)) < GAUGE_DEV
    for t in range(gauges // LANES):
        tile = dense[:, LANES * t : LANES * (t + 1)]
        turned = pltpu.roll(tile, GAUGE_DEV, 1)
        out[2 * t] = jnp.where(low, tile[:half], turned[half:])
        out[2 * t + 1] = jnp.where(low, turned[:half], tile[half:])


def finish_kernel(parts, out, *, series):
    total = parts[0]
    for k in range(1, parts.shape[0]):
        total = total + parts[k]
    turned = pltpu.roll(total, GAUGE_DEV, 1)
    out[: series // 2, :] = total[:, :GAUGE_DEV]
    out[series // 2 :, :] = turned[:, :GAUGE_DEV]


def in_vmem(count):
    return [pl.BlockSpec(memory_space=pltpu.VMEM)] * count


def in_smem(count):
    return [pl.BlockSpec(memory_space=pltpu.SMEM)] * count


def f32(*shape):
    return jax.ShapeDtypeStruct(shape, jnp.float32)


def shards(surface, east, north, east_depth, north_depth, slot_gauge, slot_cell):
    rows, cols = surface.shape
    margin = STEPS
    series = 3 * STEPS
    n_gx, n_gy = lax.axis_size("gx"), lax.axis_size("gy")
    a, b = lax.axis_index("gx"), lax.axis_index("gy")
    fields = (surface, east, north, east_depth, north_depth)

    whole = pl.BlockSpec(memory_space=pltpu.HBM)
    place_x = a.astype(jnp.int32).reshape(1)
    place_y = b.astype(jnp.int32).reshape(1)

    def bonds(count):
        links = [(i, i + 1) for i in range(1, count - 1, 2)]
        return links + [(j, i) for i, j in links]

    def pairs(count):
        return [[2 * i, 2 * i + 1] for i in range(count // 2)]

    near, far = pl.pallas_call(
        functools.partial(pack_rows_kernel, margin=margin),
        out_shape=(f32(5 * margin, cols), f32(5 * margin, cols)),
        in_specs=in_smem(1) + [whole] * 5,
        out_specs=tuple(in_vmem(2)),
        scratch_shapes=[pltpu.SemaphoreType.DMA((10,))],
        compiler_params=pltpu.CompilerParams(vmem_limit_bytes=4 * MIB),
        name="pack_rows",
    )(place_x, *(pltpu.with_memory_space_constraint(f, pltpu.HBM) for f in fields))
    row_far = lax.ppermute(far, "gx", bonds(n_gx))
    row_near = lax.all_gather(near, "gx", axis_index_groups=pairs(n_gx))

    height = rows + 2 * margin
    near, far = pl.pallas_call(
        functools.partial(pack_columns_kernel, margin=margin),
        out_shape=(f32(height, LANES), f32(height, LANES)),
        in_specs=in_smem(2) + in_vmem(7),
        out_specs=tuple(in_vmem(2)),
        compiler_params=pltpu.CompilerParams(vmem_limit_bytes=4 * MIB),
        name="pack_columns",
    )(place_x, place_y, *fields, row_near, row_far)
    from_far = lax.ppermute(far, "gy", bonds(n_gy))
    from_near = lax.all_gather(near, "gy", axis_index_groups=pairs(n_gy))

    tiles = cols // LANES + 1
    pitch = height + 8
    history = pltpu.VMEM((tiles, (STEPS + 1) * pitch, LANES), jnp.float32)
    depth = pltpu.VMEM((tiles, height, LANES), jnp.float32)
    eta, u, v, rec = pl.pallas_call(
        functools.partial(steps_kernel, steps=STEPS, last_x=n_gx - 1, last_y=n_gy - 1),
        out_shape=(f32(rows, cols),) * 3 + (f32(series + 8, LANES),),
        in_specs=[whole] + in_smem(2) + [whole] + in_vmem(9),
        out_specs=(whole,) * 3 + tuple(in_vmem(1)),
        scratch_shapes=[
            history, history, history, depth, depth, depth, depth,
            pltpu.SMEM(slot_cell.shape, jnp.int32),
            pltpu.VMEM(slot_gauge.shape, jnp.int32),
            pltpu.VMEM((rows, cols), jnp.float32),
            pltpu.SemaphoreType.DMA((2,)),
            pltpu.SemaphoreType.DMA((2 * tiles - 1,)),
        ],
        compiler_params=pltpu.CompilerParams(vmem_limit_bytes=24 * MIB),
        name="leapfrog",
    )(
        pltpu.with_memory_space_constraint(slot_cell, pltpu.HBM),
        place_x,
        place_y,
        pltpu.with_memory_space_constraint(slot_gauge, pltpu.HBM),
        *fields, row_near, row_far, from_near, from_far,
    )

    members = n_gy // 2
    chips = [[i + 2 * j for j in range(members)] for i in range(2)]
    gathered = lax.all_gather(rec, "gy", axis_index_groups=pairs(n_gy))
    base = (a * (n_gy * GAUGE_DEV) + (b % 2) * GAUGE_DEV).astype(jnp.int32).reshape(1)
    half = series // 2
    placed = pl.pallas_call(
        functools.partial(place_kernel, series=series, members=members),
        out_shape=f32(members, half, LANES),
        in_specs=in_smem(1) + in_vmem(1),
        out_specs=in_vmem(1)[0],
        compiler_params=pltpu.CompilerParams(vmem_limit_bytes=8 * MIB),
        name="place",
    )(base, gathered)
    arrived = lax.all_to_all(placed, "gy", 0, 0, axis_index_groups=chips, tiled=True)
    out = pl.pallas_call(
        functools.partial(finish_kernel, series=series),
        out_shape=f32(series, GAUGE_DEV),
        in_specs=in_vmem(1),
        out_specs=in_vmem(1)[0],
        compiler_params=pltpu.CompilerParams(vmem_limit_bytes=4 * MIB),
        name="finish",
    )(arrived)
    return eta, u, v, out.T


def solution(mesh):
    block = P("gx", "gy")
    rows = P(("gx", "gy"), None)
    return jax.shard_map(
        shards,
        mesh=mesh,
        in_specs=(block,) * 5 + (rows, rows),
        out_specs=(block,) * 3 + (rows,),
        check_vma=False,
    )
```
